32 devices in a mesh: sample: 4 (over y, x), gz: 8 (over z, core).
Axes of the slice: x: 2, y: 2, z: 4, core: 2. Of those that a mesh axis runs over, the one named last changes fastest.
Arguments:
- field_now: float32 [12, 16, 160, 256], P('sample', 'gz'), parts along dimension 0, may hold values from -6 to 6
- field_before: float32 [12, 16, 160, 256], P('sample', 'gz'), parts along dimension 0, may hold values from -6 to 6
- lame_lambda: float32 [16, 640, 256], P('gz', 'sample'), parts along dimension 1, may hold values from 0.5 to 1.5
- shear_modulus: float32 [16, 640, 256], P('gz', 'sample'), parts along dimension 1, may hold values from 0.5 to 1.5
- density: float32 [16, 640, 256], P('gz', 'sample'), parts along dimension 1, may hold values from 1 to 2
- source_field: float32 [12, 16, 160, 256], P('sample', 'gz'), parts along dimension 0, may hold values from -6 to 6
- wavelet: float32 [32], P('sample'), parts along dimension 0, may hold values from -4 to 4
- prior_mean: float32 [16, 640, 256], P('gz', 'sample'), parts along dimension 1, may hold values from 0.5 to 1.5
- steps_taken: float32 [16, 16, 160, 256], P('sample', 'gz'), parts along dimension 0
- grad_change: float32 [16, 16, 160, 256], P('sample', 'gz'), parts along dimension 0, as said below
Outputs:
- field_final: float32 [12, 16, 160, 256], P('sample', 'gz'), parts along dimension 0
- gradient: float32 [16, 640, 256], P('gz', 'sample'), parts along dimension 1
- direction: float32 [16, 640, 256], P('gz', 'sample'), parts along dimension 1
The draws below stay inside these ranges and needn't reach their ends.
There are 4 independent parts, one for each index of `sample`. The reference program is written for one: setup_inputs(seed, part) draws one part's arguments, and reference() takes and returns one part's arrays. A program takes and returns all parts, laid end to end along the dimension named above; each array names one. Nothing has to cross between parts.
Inputs may be any that keep to these rules, and one draw needn't show every extreme that they name: Each entry of grad_change is 0.5 to 2 times the matching entry of steps_taken.
All inputs are finite; a program needn't handle non-finite values.
Results may differ from the reference program's by a relative error of at most 0.0003.
Values sent between devices are 32-bit elements; how exact they have to be, the bound alone decides.
No kernel may reach another device: no remote copies, remote signals or barrier semaphores. Data moves between devices by JAX's collectives and lax.ppermute only.
A program may use at most 64 MiB of HBM per device.

```python
import math
import jax
import jax.numpy as jnp
from jax import lax

NX = 160
NY = 256
STEPS = 8
PAIRS = 4
NZ = 16


def common_model(key):
    base = jax.random.fold_in(key, 11)
    keys = jax.random.split(base, 5)
    shape = (NZ, NX, NY)
    shear = jax.random.uniform(keys[0], shape, jnp.float32, 0.5, 1.5)
    prior = jax.random.uniform(keys[1], shape, jnp.float32, 0.5, 1.5)
    levels = 1.0 + 2.0 * jnp.arange(NZ, dtype=jnp.float32) / max(NZ - 1, 1)
    noise = jax.random.normal(keys[3], (PAIRS,) + shape, jnp.float32)
    weights = jax.random.uniform(keys[2], (PAIRS, 1, 1, 1), jnp.float32, 0.5, 2.0)
    updates = levels[None, :, None, None] * (weights * (shear - prior)[None] + 0.5 * noise)
    factors = jnp.exp(jax.random.uniform(keys[4], (PAIRS,) + shape, jnp.float32, -0.6931, 0.6931))
    changes = factors * updates
    return (shear, prior, updates, changes)


def draw_shear_modulus(key, part):
    return common_model(key)[0]


def draw_prior_mean(key, part):
    return common_model(key)[1]


def draw_steps_taken(key, part):
    return common_model(key)[2]


def draw_grad_change(key, part):
    return common_model(key)[3]


def shard_levels(rng, extent, cuts, low, top_value):
    def one(dim, shards_of):
        draws = jax.random.uniform(jax.random.fold_in(jax.random.fold_in(rng, 6), dim), (shards_of,), jnp.float32, low / len(cuts), top_value / len(cuts))
        return jnp.repeat(jnp.exp(draws), extent[dim] // shards_of).reshape((-1,) + (1,) * (len(extent) - dim - 1))

    level = one(*cuts[0])
    for cut in cuts[1:]:
        level = level * one(*cut)
    return level


def gaussian(key, extent, deviation, bound, pieces=(), kind=jnp.bfloat16):
    values = jax.random.normal(key, extent, jnp.float32) * deviation
    if len(pieces) > 0:
        values = shard_levels(key, extent, pieces, -0.22, 0.18) * values
    return jnp.clip(values, min=-bound, max=bound).astype(kind)


def setup_inputs(seed: int = 0, part: int = 0) -> dict:
    arg_keys = jax.random.split(jax.random.key(seed), 11)
    part_keys = jax.random.split(jax.random.fold_in(arg_keys[10], part), 11)
    field_now = gaussian(part_keys[0], (3, NZ, NX, NY), 1.0, 6.0, ((1, 8),), jnp.float32)
    field_before = gaussian(part_keys[1], (3, NZ, NX, NY), 1.0, 6.0, ((1, 8),), jnp.float32)
    lame_lambda = jnp.clip(0.5 + 1.0 * jax.random.uniform(part_keys[2], (NZ, NX, NY), jnp.float32) ** shard_levels(part_keys[2], (NZ, NX, NY), ((0, 8),), -0.2, 0.2), 0.5, 1.5)
    shear_modulus = draw_shear_modulus(jax.random.fold_in(jax.random.fold_in(arg_keys[10], part), 71), part)
    density = jnp.clip(jnp.exp(math.log(2.0) - 0.6931472 * jax.random.uniform(part_keys[4], (NZ, NX, NY), jnp.float32) ** shard_levels(part_keys[4], (NZ, NX, NY), ((0, 8),), -0.2, 0.2)), 1.0, 2.0)
    source_field = gaussian(part_keys[5], (3, NZ, NX, NY), 1.0, 6.0, ((1, 8),), jnp.float32)
    wavelet = gaussian(part_keys[6], (STEPS,), 1.0, 4.0, (), jnp.float32)
    prior_mean = draw_prior_mean(jax.random.fold_in(jax.random.fold_in(arg_keys[10], part), 71), part)
    steps_taken = draw_steps_taken(jax.random.fold_in(jax.random.fold_in(arg_keys[10], part), 71), part)
    grad_change = draw_grad_change(jax.random.fold_in(jax.random.fold_in(arg_keys[10], part), 71), part)
    return {"field_now": field_now, "field_before": field_before, "lame_lambda": lame_lambda, "shear_modulus": shear_modulus, "density": density, "source_field": source_field, "wavelet": wavelet, "prior_mean": prior_mean, "steps_taken": steps_taken, "grad_change": grad_change}


def shifted(padded, comp, offset):
    depth = padded.shape[1] - 2
    rows = padded.shape[2] - 2
    cols = padded.shape[3] - 2
    return lax.slice(padded[comp], (1 + offset[0], 1 + offset[1], 1 + offset[2]), (1 + offset[0] + depth, 1 + offset[1] + rows, 1 + offset[2] + cols))


def vec_add(first, second):
    return (first[0] + second[0], first[1] + second[1], first[2] + second[2])


def vec_neg(first):
    return (-first[0], -first[1], -first[2])


def operate(extended, lame_first, shear):
    padded = jnp.pad(extended, ((0, 0), (0, 0), (1, 1), (1, 1)))
    units = ((1, 0, 0), (0, 1, 0), (0, 0, 1))
    centre = (0, 0, 0)
    seconds = [[shifted(padded, comp, units[axis]) + shifted(padded, comp, vec_neg(units[axis])) - 2.0 * shifted(padded, comp, centre) for axis in range(3)] for comp in range(3)]

    def mixed(comp, first, second):
        plus_first = units[first]
        plus_second = units[second]
        return 0.25 * (shifted(padded, comp, vec_add(plus_first, plus_second)) - shifted(padded, comp, vec_add(plus_first, vec_neg(plus_second))) - shifted(padded, comp, vec_add(vec_neg(plus_first), plus_second)) + shifted(padded, comp, vec_neg(vec_add(plus_first, plus_second))))

    laplace = []
    elastic = []
    for comp in range(3):
        lap_comp = seconds[comp][0] + seconds[comp][1] + seconds[comp][2]
        grad_div = seconds[comp][comp]
        for other in range(3):
            if other != comp:
                grad_div = grad_div + mixed(other, comp, other)
        laplace.append(lap_comp)
        elastic.append((lame_first + shear) * grad_div + shear * lap_comp)
    return jnp.stack(elastic), jnp.stack(laplace)


def reference(field_now, field_before, lame_lambda, shear_modulus, density, source_field, wavelet, prior_mean, steps_taken, grad_change):
    coeff = 0.04 / density
    current = field_now
    earlier = field_before
    correlation = jnp.zeros(shear_modulus.shape, jnp.float32)
    for step in range(STEPS):
        extended = jnp.pad(current, ((0, 0), (1, 1), (0, 0), (0, 0)))
        elastic, laplace = operate(extended, lame_lambda, shear_modulus)
        correlation = correlation + jnp.sum(current * laplace, axis=0)
        nxt = 2.0 * current - earlier + coeff * (elastic + wavelet[step] * source_field)
        earlier = current
        current = nxt
    gradient = (shear_modulus - prior_mean) + 0.02 * correlation
    curv = [jnp.sum(steps_taken[i] * grad_change[i]) for i in range(PAIRS)]
    query = gradient
    alphas = [None] * PAIRS
    for i in reversed(range(PAIRS)):
        alphas[i] = jnp.sum(steps_taken[i] * query) / curv[i]
        query = query - alphas[i] * grad_change[i]
    newest = grad_change[PAIRS - 1]
    result = (curv[PAIRS - 1] / jnp.sum(newest * newest)) * query
    for i in range(PAIRS):
        beta = jnp.sum(grad_change[i] * result) / curv[i]
        result = result + (alphas[i] - beta) * steps_taken[i]
    return current, gradient, -result
```

```python
import functools

import jax
import jax.numpy as jnp
from jax import lax
from jax.experimental import pallas as pl
from jax.experimental.pallas import tpu as pltpu
from jax.sharding import PartitionSpec as P

STEPS = 8
PAIRS = 4
ROWS = 8
LANES = 128
AXES = ("sample", "gz")
DOTS = [("s", i, j) for i in range(PAIRS) for j in range(i, PAIRS)] + [
    ("y", i, j) for i in range(PAIRS) for j in range(i, PAIRS)
]
DOT_ROWS = 32

VMEM = pl.BlockSpec(memory_space=pltpu.VMEM)
SMEM = pl.BlockSpec(memory_space=pltpu.SMEM)


def mul(x, y):
    return [a * b for a, b in zip(x, y)]


def add(x, y):
    return [a + b for a, b in zip(x, y)]


def sub(x, y):
    return [a - b for a, b in zip(x, y)]


def scale(x, factor):
    return [a * factor for a in x]


def lanes_of(ref, index, tile):
    row = tile * ROWS if isinstance(tile, int) else pl.multiple_of(tile * ROWS, ROWS)
    count = ref.shape[-1] // LANES
    return [ref[(*index, pl.ds(row, ROWS), pl.ds(k * LANES, LANES))] for k in range(count)]


def store(ref, index, tile, values):
    row = tile * ROWS if isinstance(tile, int) else pl.multiple_of(tile * ROWS, ROWS)
    for k, value in enumerate(values):
        ref[(*index, pl.ds(row, ROWS), pl.ds(k * LANES, LANES))] = value


def along_y(x, lane):
    up = [pltpu.roll(a, LANES - 1, 1) for a in x]
    down = [pltpu.roll(a, 1, 1) for a in x]
    count = len(x)
    zero = jnp.zeros_like(x[0])
    high = [
        jnp.where(lane == LANES - 1, up[k + 1] if k + 1 < count else zero, up[k])
        for k in range(count)
    ]
    low = [jnp.where(lane == 0, down[k - 1] if k > 0 else zero, down[k]) for k in range(count)]
    return high, low


def along_x(before, here, after, row, first, last):
    high, low = [], []
    for b, h, a in zip(before, here, after):
        high.append(
            jnp.where(row == ROWS - 1, pltpu.roll(a, ROWS - 1, 0) * last, pltpu.roll(h, ROWS - 1, 0))
        )
        low.append(jnp.where(row == 0, pltpu.roll(b, 1, 0) * first, pltpu.roll(h, 1, 0)))
    return high, low


def plane_update(centre, ici, d2d, quarter, row, lane, first, last):
    u = [[centre(c, k) for k in (-1, 0, 1)] for c in range(3)]
    i0, d0 = [ici(c, 0) for c in range(3)], [d2d(c, 0) for c in range(3)]
    w = [scale(sub(i0[c], d0[c]), quarter) for c in range(3)]
    w1 = [scale(sub(ici(1, k), d2d(1, k)), quarter) if k else w[1] for k in (-1, 0, 1)]
    w0 = [scale(sub(ici(0, k), d2d(0, k)), quarter) if k else w[0] for k in (-1, 0, 1)]
    y2 = [along_y(u[2][k], lane) for k in range(3)]
    g1 = [add(w0[k], scale(sub(*y2[k]), 0.25)) for k in range(3)]
    xs = [along_x(*u[c], row, first, last) for c in range(3)]
    ys = [along_y(u[0][1], lane), along_y(u[1][1], lane), y2[1]]
    xw1 = along_x(*w1, row, first, last)
    xg1 = along_x(*g1, row, first, last)
    yw2 = along_y(w[2], lane)
    g2 = add(w[0], scale(sub(*xs[1]), 0.25))
    yg2 = along_y(g2, lane)
    twice = [scale(u[c][1], 2.0) for c in range(3)]
    second = [
        [
            sub(add(i0[c], d0[c]), twice[c]),
            sub(add(*xs[c]), twice[c]),
            sub(add(*ys[c]), twice[c]),
        ]
        for c in range(3)
    ]
    lap = [add(add(second[c][0], second[c][1]), second[c][2]) for c in range(3)]
    grad_div = [
        add(second[0][0], add(sub(*xw1), sub(*yw2))),
        add(second[1][1], sub(*xg1)),
        add(second[2][2], sub(*yg2)),
    ]
    return [u[c][1] for c in range(3)], twice, grad_div, lap


def step_kernel(step, start, stop, total, splits, parts, ip, fs, *refs):
    names = ["h", "q", "p", "f", "pb", "fb"] + ([] if step == 0 else ["corr"])
    source = {}
    at = 0
    for name in names:
        source[name] = refs[at : at + parts]
        at += parts
    ca, cb, cf, src = refs[at : at + 4]
    p_out, f_out, corr_out = refs[at + 4 :]
    near = ip[0]
    quarter = fs[0]
    present = fs[1]
    wave = fs[2 + step]
    row = lax.broadcasted_iota(jnp.int32, (ROWS, LANES), 0)
    lane = lax.broadcasted_iota(jnp.int32, (ROWS, LANES), 1)

    def tile_body(t, static):
        if static:
            first = 0.0 if t == 0 else 1.0
            last = 0.0 if t == total - 1 else 1.0
        else:
            first = jnp.where(t == 0, 0.0, 1.0)
            last = jnp.where(t == total - 1, 0.0, 1.0)

        def read(name, index, k):
            n = t + k
            n = min(max(n, 0), total - 1) if static else jnp.clip(n, 0, total - 1)
            held = source[name]
            if parts == 1:
                return lanes_of(held[0], index, n)
            if static and n < splits[name]:
                return lanes_of(held[0], index, n)
            return lanes_of(held[1], index, n - splits[name])

        def reader(name):
            if name == "h":
                return lambda c, k: scale(read("h", (c,), k), present)
            return lambda c, k: read(name, (c,), k)

        work = ((near, 0, "phf", "pb", p_out), (1 - near, 1, "fpq", "fb", f_out))
        for index, slot, three, older, out in work:
            centre, ici, d2d = (reader(name) for name in three)
            here, twice, grad_div, lap = plane_update(
                centre, ici, d2d, quarter, row, lane, first, last
            )
            a, b = lanes_of(ca, (index,), t), lanes_of(cb, (index,), t)
            force = scale(lanes_of(cf, (index,), t), wave)
            product = None if step == 0 else read("corr", (slot,), 0)
            for c in range(3):
                term = mul(here[c], lap[c])
                product = term if product is None else add(product, term)
                new = sub(twice[c], read(older, (c,), 0))
                new = add(new, mul(force, lanes_of(src, (c, index), t)))
                new = add(new, add(mul(a, grad_div[c]), mul(b, lap[c])))
                store(out, (c,), t - start, new)
            store(corr_out, (slot,), t - start, product)

    begin = start
    if parts == 2:
        begin = min(max(splits.values()), stop)
        for t in range(start, begin):
            tile_body(t, True)
    if begin < stop:

        def loop(t, carry):
            tile_body(t, False)
            return carry

        lax.fori_loop(begin, stop, loop, 0)


def step_call(step, start, stop, total, splits, ints, floats, held, fixed, name):
    operands = [ints, floats] + held + fixed
    cols = held[0].shape[-1]
    rows = (stop - start) * ROWS
    names = 6 if step == 0 else 7
    return call(
        functools.partial(step_kernel, step, start, stop, total, splits, len(held) // names),
        [(3, rows, cols), (3, rows, cols), (2, rows, cols)],
        operands,
        rows * cols * 240,
        name,
        2,
    )


VMEM_LIMIT = 20 * 2**20


def split_kernel(cut, ip, u, *outs):
    near = ip[0]
    rows = u.shape[2]
    for index, (low, high) in ((near, outs[:2]), (1 - near, outs[2:])):
        for c in range(3):
            low[c] = u[c, index, pl.ds(0, cut), :]
            high[c] = u[c, index, pl.ds(cut, rows - cut), :]


def join_kernel(ip, p_low, p_high, f_low, f_high, out):
    near = ip[0]
    cut, rest = p_low.shape[1], p_high.shape[1]
    for index, low, high in ((near, p_low, p_high), (1 - near, f_low, f_high)):
        for c in range(3):
            out[c, index, pl.ds(0, cut), :] = low[c]
            out[c, index, pl.ds(cut, rest), :] = high[c]


def coeff_kernel(lam, mu, rho, ca, cb, cf):
    rows = lam.shape[1] // ROWS

    def loop(t, carry):
        r = pl.ds(pl.multiple_of(t * ROWS, ROWS), ROWS)
        for d in range(lam.shape[0]):
            coeff = 0.04 / rho[d, r, :]
            m = mu[d, r, :]
            ca[d, r, :] = coeff * (lam[d, r, :] + m)
            cb[d, r, :] = coeff * m
            cf[d, r, :] = coeff
        return carry

    lax.fori_loop(0, rows, loop, 0)


def dots_kernel(s, y, out):
    depth, rows, cols = s.shape[1:]
    count = len(DOTS)

    def loop(t, sums):
        r = pl.ds(pl.multiple_of(t * ROWS, ROWS), ROWS)
        sums = list(sums)
        for d in range(depth):
            for k in range(cols // LANES):
                at = (d, r, pl.ds(k * LANES, LANES))
                vs = [s[(i, *at)] for i in range(PAIRS)]
                vy = [y[(i, *at)] for i in range(PAIRS)]
                for n, (kind, i, j) in enumerate(DOTS):
                    sums[n] = sums[n] + (vs[i] if kind == "s" else vy[i]) * vy[j]
        return tuple(sums)

    zero = jnp.zeros((ROWS, LANES), jnp.float32)
    sums = lax.fori_loop(0, rows // ROWS, loop, (zero,) * count)
    out[...] = jnp.zeros(out.shape, jnp.float32)
    for n in range(count):
        out[pl.ds(n, 1), :] = jnp.sum(sums[n], axis=0, keepdims=True)


def gradient_kernel(ip, corr_low, corr_high, mu, prior, s, y, static, grad, out):
    near = ip[0]
    cols = mu.shape[2]
    sums = (jnp.zeros((ROWS, LANES), jnp.float32),) * (2 * PAIRS)
    base = 0
    for corr in (corr_low, corr_high):

        def loop(t, sums, corr=corr, base=base):
            sums = list(sums)
            r = pl.ds(pl.multiple_of((base + t) * ROWS, ROWS), ROWS)
            r_corr = pl.ds(pl.multiple_of(t * ROWS, ROWS), ROWS)
            for slot, index in ((0, near), (1, 1 - near)):
                for k in range(cols // LANES):
                    lanes = pl.ds(k * LANES, LANES)
                    at = (index, r, lanes)
                    g = (mu[at] - prior[at]) + 0.02 * corr[slot, r_corr, lanes]
                    grad[at] = g
                    for i in range(PAIRS):
                        sums[i] = sums[i] + s[(i, *at)] * g
                        sums[PAIRS + i] = sums[PAIRS + i] + y[(i, *at)] * g
            return tuple(sums)

        tiles = corr.shape[1] // ROWS
        sums = lax.fori_loop(0, tiles, loop, sums)
        base += tiles
    out[...] = static[...]
    for n in range(2 * PAIRS):
        out[pl.ds(len(DOTS) + n, 1), :] = jnp.sum(sums[n], axis=0, keepdims=True)


def direction_kernel(parts, grad, s, y, out):
    depth, rows, cols = grad.shape
    dots = parts[0]
    for n in range(1, parts.shape[0]):
        dots = dots + parts[n]
    shift = LANES // 2
    while shift:
        dots = dots + pltpu.roll(dots, shift, 1)
        shift //= 2
    value = {}
    for n, key in enumerate(DOTS):
        value[key] = dots[n : n + 1, :]
    for i in range(PAIRS):
        value["sg", i] = dots[len(DOTS) + i : len(DOTS) + i + 1, :]
        value["yg", i] = dots[len(DOTS) + PAIRS + i : len(DOTS) + PAIRS + i + 1, :]
    rho = [1.0 / value["s", i, i] for i in range(PAIRS)]
    alpha = [None] * PAIRS
    for i in reversed(range(PAIRS)):
        inner = value["sg", i]
        for j in range(i + 1, PAIRS):
            inner = inner - alpha[j] * value["s", i, j]
        alpha[i] = rho[i] * inner
    last = PAIRS - 1
    gamma = value["s", last, last] / value["y", last, last]
    step = [None] * PAIRS
    for i in range(PAIRS):
        inner = value["yg", i]
        for j in range(PAIRS):
            inner = inner - alpha[j] * value["y", min(i, j), max(i, j)]
        inner = gamma * inner
        for j in range(i):
            inner = inner + step[j] * value["s", j, i]
        step[i] = alpha[i] - rho[i] * inner
    wide = lambda x: jnp.broadcast_to(x, (ROWS, LANES))
    by_g = wide(-gamma)
    by_y = [wide(gamma * a) for a in alpha]
    by_s = [wide(-b) for b in step]

    def loop(t, carry):
        r = pl.ds(pl.multiple_of(t * ROWS, ROWS), ROWS)
        for d in range(depth):
            for k in range(cols // LANES):
                at = (d, r, pl.ds(k * LANES, LANES))
                total = by_g * grad[at]
                for i in range(PAIRS):
                    total = total + by_y[i] * y[(i, *at)] + by_s[i] * s[(i, *at)]
                out[at] = total
        return carry

    lax.fori_loop(0, rows // ROWS, loop, 0)


def call(kernel, out_shape, operands, flops, name, smem=0):
    return pl.pallas_call(
        kernel,
        out_shape=[jax.ShapeDtypeStruct(x, jnp.float32) for x in out_shape],
        in_specs=[SMEM] * smem + [VMEM] * (len(operands) - smem),
        out_specs=[VMEM] * len(out_shape),
        compiler_params=pltpu.CompilerParams(vmem_limit_bytes=VMEM_LIMIT),
        cost_estimate=pl.CostEstimate(flops=flops, bytes_accessed=0, transcendentals=0),
        name=name,
    )(*operands)


def pairings():
    samples, count = lax.axis_size("sample"), lax.axis_size("gz")
    inside = [(i, i ^ 1) for i in range(count)]
    across = []
    for sample in range(samples):
        for i in range(1, count - 1, 2):
            across += [(sample * count + i, sample * count + i + 1)]
            across += [(sample * count + i + 1, sample * count + i)]
        partner = sample ^ 1 if samples % 2 == 0 else sample
        for i in (0, count - 1):
            across.append((sample * count + i, partner * count + i))
    return inside, across


def sum_over_gz(part):
    count = lax.axis_size("gz")
    pair = part + lax.ppermute(part, "gz", [(i, i ^ 1) for i in range(count)])
    if count > 8:
        return lax.psum(part, "gz")[None]
    parts = [pair]
    for k in range(1, count // 2):
        parts.append(lax.ppermute(pair, "gz", [(i, (i + 2 * k) % count) for i in range(count)]))
    return jnp.stack(parts)


def on_device(
    field_now,
    field_before,
    lame_lambda,
    shear_modulus,
    density,
    source_field,
    wavelet,
    prior_mean,
    steps_taken,
    grad_change,
):
    depth, rows, cols = shear_modulus.shape
    count = lax.axis_size("gz")
    assert depth == 2 and count % 2 == 0
    inside, across = pairings()
    total = rows // ROWS
    cells = shear_modulus.size
    cuts = [total // 2 + STEPS // 2 - n for n in range(STEPS + 1)]
    place = lax.axis_index("gz")
    near = place % 2
    ints = jnp.reshape(near, (1,)).astype(jnp.int32)
    sign = jnp.where(near == 1, 0.25, -0.25)
    present = jnp.where((place == 0) | (place == count - 1), 0.0, 1.0)
    floats = jnp.concatenate([jnp.stack([sign, present]).astype(jnp.float32), wavelet])

    def cut_planes(field, tiles, name):
        cut = tiles * ROWS
        shapes = [(3, cut, cols), (3, rows - cut, cols)] * 2
        outs = call(functools.partial(split_kernel, cut), shapes, [ints, field], cells, name, 1)
        return outs[:2], outs[2:]

    now = cut_planes(field_now, cuts[0], "cut_now")
    older = cut_planes(field_before, cuts[0] + 1, "cut_before")
    fixed = call(
        coeff_kernel,
        [shear_modulus.shape] * 3,
        [lame_lambda, shear_modulus, density],
        cells * 10,
        "coeffs",
    )
    fixed = list(fixed) + [source_field]
    (static,) = call(
        dots_kernel, [(DOT_ROWS, LANES)], [steps_taken, grad_change], cells * 40, "static_dots"
    )
    swap_b = lambda x: lax.ppermute(x, AXES, across)
    swap_a = lambda x: lax.ppermute(x, "gz", inside)
    ghosts = [[swap_b(now[0][i]), swap_a(now[1][i])] for i in range(2)]
    ghosts = list(zip(*ghosts))
    corr = None
    for n in range(STEPS):
        last = n == STEPS - 1
        middle = cuts[n + 1]
        groups = [*ghosts, *now, *older] + ([] if n == 0 else [corr])
        splits = {k: cuts[n] for k in ("h", "q", "p", "f", "corr")}
        splits |= {k: cuts[n] + 1 for k in ("pb", "fb")}
        args = (ints, floats)
        p_low, f_low, corr_low = step_call(
            n, 0, middle, total, splits, *args, [g[0] for g in groups], fixed, f"step{n}_low"
        )
        if not last:
            low_ghosts = [swap_b(p_low), swap_a(f_low)]
        both = [x for g in groups for x in g]
        p_high, f_high, corr_high = step_call(
            n, middle, total, total, splits, *args, both, fixed, f"step{n}_high"
        )
        if not last:
            ghosts = list(zip(low_ghosts, [swap_b(p_high), swap_a(f_high)]))
        older, now = now, ((p_low, p_high), (f_low, f_high))
        corr = (corr_low, corr_high)
    gradient, mine = call(
        gradient_kernel,
        [shear_modulus.shape, (DOT_ROWS, LANES)],
        [ints, *corr, shear_modulus, prior_mean, steps_taken, grad_change, static],
        cells * 20,
        "gradient",
        1,
    )
    (final,) = call(
        join_kernel, [field_now.shape], [ints, *now[0], *now[1]], cells, "join", 1
    )
    parts = sum_over_gz(mine)
    (direction,) = call(
        direction_kernel,
        [shear_modulus.shape],
        [parts, gradient, steps_taken, grad_change],
        cells * 20,
        "direction",
    )
    return (final, gradient, direction)


def solution(mesh):
    placed = (
        P("sample", "gz", None, None),
        P("sample", "gz", None, None),
        P("gz", "sample", None),
        P("gz", "sample", None),
        P("gz", "sample", None),
        P("sample", "gz", None, None),
        P("sample"),
        P("gz", "sample", None),
        P("sample", "gz", None, None),
        P("sample", "gz", None, None),
    )
    return jax.shard_map(
        on_device,
        mesh=mesh,
        in_specs=placed,
        out_specs=(P("sample", "gz", None, None), P("gz", "sample", None), P("gz", "sample", None)),
        check_vma=False,
    )
```

```python
import functools

import jax
import jax.numpy as jnp
from jax import lax
from jax.experimental import pallas as pl
from jax.experimental.pallas import tpu as pltpu
from jax.sharding import PartitionSpec as P


STEPS = 8
PAIRS = 4
ROWS = 8
LANES = 128
AXES = ("sample", "gz")
DOTS = [("s", i, j) for i in range(PAIRS) for j in range(i, PAIRS)] + [
    ("y", i, j) for i in range(PAIRS) for j in range(i, PAIRS)
]
DOT_ROWS = 32

VMEM = pl.BlockSpec(memory_space=pltpu.VMEM)


def near_plane():
    return lax.rem(lax.axis_index("gz"), 2)


def has_chip_neighbour():
    place = lax.axis_index("gz")
    edge = (place == 0) | (place == lax.axis_size("gz") - 1)
    return jnp.where(edge, 0.0, 1.0).astype(jnp.float32)


def mul(x, y):
    return [a * b for a, b in zip(x, y)]


def add(x, y):
    return [a + b for a, b in zip(x, y)]


def sub(x, y):
    return [a - b for a, b in zip(x, y)]


def scale(x, factor):
    return [a * factor for a in x]


def lanes_of(ref, index, tile):
    row = tile * ROWS if isinstance(tile, int) else pl.multiple_of(tile * ROWS, ROWS)
    count = ref.shape[-1] // LANES
    return [ref[(*index, pl.ds(row, ROWS), pl.ds(k * LANES, LANES))] for k in range(count)]


def store(ref, index, tile, values):
    row = tile * ROWS if isinstance(tile, int) else pl.multiple_of(tile * ROWS, ROWS)
    for k, value in enumerate(values):
        ref[(*index, pl.ds(row, ROWS), pl.ds(k * LANES, LANES))] = value


def along_y(x, lane):
    zero = jnp.zeros_like(x[0])
    after = x[1:] + [zero]
    before = [zero] + x[:-1]
    high = [pltpu.roll(jnp.where(lane == 0, a, h), LANES - 1, 1) for a, h in zip(after, x)]
    low = [pltpu.roll(jnp.where(lane == LANES - 1, b, h), 1, 1) for b, h in zip(before, x)]
    return high, low


def along_x(before, here, after, row):
    high = [pltpu.roll(jnp.where(row == 0, a, h), ROWS - 1, 0) for a, h in zip(after, here)]
    low = [pltpu.roll(jnp.where(row == ROWS - 1, b, h), 1, 0) for b, h in zip(before, here)]
    return high, low


def plane_update(centre, ici, d2d, quarter, row, lane):
    u = [centre(c, 0) for c in range(3)]
    i0, d0 = [ici(c, 0) for c in range(3)], [d2d(c, 0) for c in range(3)]
    v = [sub(i0[c], d0[c]) for c in range(3)]
    xv = [
        along_x(sub(ici(c, -1), d2d(c, -1)), v[c], sub(ici(c, 1), d2d(c, 1)), row)
        for c in range(2)
    ]
    xs = [along_x(centre(c, -1), u[c], centre(c, 1), row) for c in range(3)]
    ys = [along_y(u[c], lane) for c in range(3)]
    yv2 = along_y(v[2], lane)
    g2 = add(scale(v[0], quarter), scale(sub(*xs[1]), 0.25))
    yg2 = along_y(g2, lane)
    yxu2 = along_y(sub(*xs[2]), lane)
    twice = [scale(u[c], 2.0) for c in range(3)]
    zsum = [add(i0[c], d0[c]) for c in range(3)]
    xsum = [add(*xs[c]) for c in range(3)]
    ysum = [add(*ys[c]) for c in range(3)]
    lap = [sub(add(add(zsum[c], xsum[c]), ysum[c]), scale(u[c], 6.0)) for c in range(3)]
    grad_div = [
        add(sub(zsum[0], twice[0]), scale(add(sub(*xv[1]), sub(*yv2)), quarter)),
        add(
            sub(xsum[1], twice[1]),
            add(scale(sub(*xv[0]), quarter), scale(sub(*yxu2), 0.25)),
        ),
        add(sub(ysum[2], twice[2]), sub(*yg2)),
    ]
    return u, twice, grad_div, lap


REACH = {"h": 1, "p": 1, "f": 1, "q": 1, "pb": 0, "fb": 0, "cp": 0, "cf": 0}


def plan(names, starts, start, stop, total):
    def sides(t):
        if t in (0, total - 1):
            return None
        found = {}
        for name in names:
            parts = starts[name]
            held = {
                max(i for i, first in enumerate(parts) if first <= t + k)
                for k in range(-REACH[name], REACH[name] + 1)
            }
            if len(held) > 1:
                return None
            found[name] = held.pop()
        return found

    runs = []
    for t in range(start, stop):
        here = sides(t)
        if here is not None and runs and runs[-1][2] == here:
            runs[-1][1] = t + 1
        else:
            runs.append([t, t + 1, here])
    return runs


def step_kernel(step, far, starts, start, stop, total, wave_ref, *refs):
    names = list(starts)
    source = {}
    at = 0
    for name in names:
        source[name] = refs[at : at + len(starts[name])]
        at += len(starts[name])
    ca, cb, cf, src = refs[at : at + 4]
    out, corr_out, token = refs[-3:]
    near = near_plane()
    index = 1 - near if far else near
    quarter, present = near.astype(jnp.float32) * 0.5 - 0.25, has_chip_neighbour()
    wave = wave_ref[step]
    row = lax.broadcasted_iota(jnp.int32, (ROWS, LANES), 0)
    lane = lax.broadcasted_iota(jnp.int32, (ROWS, LANES), 1)
    zeros = [jnp.zeros((ROWS, LANES), jnp.float32)] * (out.shape[2] // LANES)

    def tile_body(t, where):
        def read(name, at, k):
            n = t + k
            if where is None:
                if n < 0 or n >= total:
                    return zeros
                part = max(i for i, first in enumerate(starts[name]) if first <= n)
            else:
                part = where[name]
            return lanes_of(source[name][part], at, n - starts[name][part])

        def reader(name):
            if name == "h":
                return lambda c, k: scale(read("h", (c,), k), present)
            return lambda c, k: read(name, (c,), k)

        three, older, sums = ("fpq", "fb", "cf") if far else ("phf", "pb", "cp")
        here, twice, grad_div, lap = plane_update(
            *(reader(name) for name in three), quarter, row, lane
        )
        a, b = lanes_of(ca, (index,), t), lanes_of(cb, (index,), t)
        force = scale(lanes_of(cf, (index,), t), wave)
        product = None if step == 0 else read(sums, (), 0)
        for c in range(3):
            term = mul(here[c], lap[c])
            product = term if product is None else add(product, term)
            new = sub(twice[c], read(older, (c,), 0))
            new = add(new, mul(force, lanes_of(src, (c, index), t)))
            new = add(new, add(mul(a, grad_div[c]), mul(b, lap[c])))
            store(out, (c,), t - start, new)
        store(corr_out, (), t - start, product)

    for first, end, where in plan(names, starts, start, stop, total):
        if end - first < 3:
            for t in range(first, end):
                tile_body(t, where)
        else:

            def loop(t, carry, where=where):
                tile_body(t, where)
                return carry

            lax.fori_loop(first, end, loop, 0, unroll=UNROLL)
    token[...] = jnp.zeros(token.shape, jnp.float32)


UNROLL = 4


def step_call(step, far, start, stop, total, held, wave, fixed, tokens):
    starts = {key: [first for first, _ in parts] for key, parts in held.items()}
    arrays = [array for parts in held.values() for _, array in parts]
    cols = arrays[0].shape[-1]
    rows = (stop - start) * ROWS
    return call(
        functools.partial(step_kernel, step, far, starts, start, stop, total),
        [(3, rows, cols), (rows, cols), (ROWS, LANES)],
        [wave, *arrays, *fixed, *tokens],
        rows * cols * 120,
    )


VMEM_LIMIT = 20 * 2**20


def split_kernel(cut, u, low, high, far):
    near = near_plane()
    rows = u.shape[2]
    for c in range(3):
        low[c] = u[c, near, pl.ds(0, cut), :]
        high[c] = u[c, near, pl.ds(cut, rows - cut), :]
        far[c] = u[c, 1 - near]


def join_kernel(p_low, p_high, f, c_low, c_high, c_f, mu, prior, out, grad):
    near = near_plane()
    cut, rest = p_low.shape[1], p_high.shape[1]
    low, high = pl.ds(0, cut), pl.ds(cut, rest)
    for c in range(3):
        out[c, near, low, :] = p_low[c]
        out[c, near, high, :] = p_high[c]
        out[c, 1 - near] = f[c]
    grad[near, low, :] = (mu[near, low, :] - prior[near, low, :]) + 0.02 * c_low[...]
    grad[near, high, :] = (mu[near, high, :] - prior[near, high, :]) + 0.02 * c_high[...]
    grad[1 - near] = (mu[1 - near] - prior[1 - near]) + 0.02 * c_f[...]


def coeff_kernel(lam, mu, rho, ca, cb, cf):
    rows = lam.shape[1] // ROWS

    def loop(t, carry):
        r = pl.ds(pl.multiple_of(t * ROWS, ROWS), ROWS)
        for d in range(lam.shape[0]):
            coeff = 0.04 / rho[d, r, :]
            m = mu[d, r, :]
            ca[d, r, :] = coeff * (lam[d, r, :] + m)
            cb[d, r, :] = coeff * m
            cf[d, r, :] = coeff
        return carry

    lax.fori_loop(0, rows, loop, 0)


def dots_kernel(s, y, out):
    depth, rows, cols = s.shape[1:]
    count = len(DOTS)

    def loop(t, sums):
        r = pl.ds(pl.multiple_of(t * ROWS, ROWS), ROWS)
        sums = list(sums)
        for d in range(depth):
            for k in range(cols // LANES):
                at = (d, r, pl.ds(k * LANES, LANES))
                vs = [s[(i, *at)] for i in range(PAIRS)]
                vy = [y[(i, *at)] for i in range(PAIRS)]
                for n, (kind, i, j) in enumerate(DOTS):
                    sums[n] = sums[n] + (vs[i] if kind == "s" else vy[i]) * vy[j]
        return tuple(sums)

    zero = jnp.zeros((ROWS, LANES), jnp.float32)
    sums = lax.fori_loop(0, rows // ROWS, loop, (zero,) * count)
    out[...] = jnp.zeros(out.shape, jnp.float32)
    for n in range(count):
        out[pl.ds(n, 1), :] = jnp.sum(sums[n], axis=0, keepdims=True)


def gradient_dots_kernel(parts, mu, prior, s, y, so_far, *refs):
    out = refs[-1]
    cols = mu.shape[2]
    sums = (jnp.zeros((ROWS, LANES), jnp.float32),) * (2 * PAIRS)
    for (far, base), corr in zip(parts, refs):
        index = 1 - near_plane() if far else near_plane()

        def loop(t, sums, corr=corr, base=base, index=index):
            sums = list(sums)
            r = pl.ds(pl.multiple_of((base + t) * ROWS, ROWS), ROWS)
            r_corr = pl.ds(pl.multiple_of(t * ROWS, ROWS), ROWS)
            for k in range(cols // LANES):
                lanes = pl.ds(k * LANES, LANES)
                at = (index, r, lanes)
                g = (mu[at] - prior[at]) + 0.02 * corr[r_corr, lanes]
                for i in range(PAIRS):
                    sums[i] = sums[i] + s[(i, *at)] * g
                    sums[PAIRS + i] = sums[PAIRS + i] + y[(i, *at)] * g
            return tuple(sums)

        sums = lax.fori_loop(0, corr.shape[0] // ROWS, loop, sums, unroll=2)
    out[...] = so_far[...]
    for n in range(2 * PAIRS):
        at = pl.ds(len(DOTS) + n, 1)
        out[at, :] = so_far[at, :] + jnp.sum(sums[n], axis=0, keepdims=True)


def direction_kernel(parts, grad, s, y, out):
    depth, rows, cols = grad.shape
    dots = parts[0]
    for n in range(1, parts.shape[0]):
        dots = dots + parts[n]
    shift = LANES // 2
    while shift:
        dots = dots + pltpu.roll(dots, shift, 1)
        shift //= 2
    value = {}
    for n, key in enumerate(DOTS):
        value[key] = dots[n : n + 1, :]
    for i in range(PAIRS):
        value["sg", i] = dots[len(DOTS) + i : len(DOTS) + i + 1, :]
        value["yg", i] = dots[len(DOTS) + PAIRS + i : len(DOTS) + PAIRS + i + 1, :]
    rho = [1.0 / value["s", i, i] for i in range(PAIRS)]
    alpha = [None] * PAIRS
    for i in reversed(range(PAIRS)):
        inner = value["sg", i]
        for j in range(i + 1, PAIRS):
            inner = inner - alpha[j] * value["s", i, j]
        alpha[i] = rho[i] * inner
    last = PAIRS - 1
    gamma = value["s", last, last] / value["y", last, last]
    step = [None] * PAIRS
    for i in range(PAIRS):
        inner = value["yg", i]
        for j in range(PAIRS):
            inner = inner - alpha[j] * value["y", min(i, j), max(i, j)]
        inner = gamma * inner
        for j in range(i):
            inner = inner + step[j] * value["s", j, i]
        step[i] = alpha[i] - rho[i] * inner
    wide = lambda x: jnp.broadcast_to(x, (ROWS, LANES))
    by_g = wide(-gamma)
    by_y = [wide(gamma * a) for a in alpha]
    by_s = [wide(-b) for b in step]

    def loop(t, carry):
        r = pl.ds(pl.multiple_of(t * ROWS, ROWS), ROWS)
        for d in range(depth):
            for k in range(cols // LANES):
                at = (d, r, pl.ds(k * LANES, LANES))
                total = by_g * grad[at]
                for i in range(PAIRS):
                    total = total + by_y[i] * y[(i, *at)] + by_s[i] * s[(i, *at)]
                out[at] = total
        return carry

    lax.fori_loop(0, rows // ROWS, loop, 0)


def call(kernel, out_shape, operands, flops):
    return pl.pallas_call(
        kernel,
        out_shape=[jax.ShapeDtypeStruct(x, jnp.float32) for x in out_shape],
        in_specs=[VMEM] * len(operands),
        out_specs=[VMEM] * len(out_shape),
        compiler_params=pltpu.CompilerParams(vmem_limit_bytes=VMEM_LIMIT),
        cost_estimate=pl.CostEstimate(flops=flops, bytes_accessed=0, transcendentals=0),
    )(*operands)


def pairings():
    samples, count = lax.axis_size("sample"), lax.axis_size("gz")
    inside = [(i, i ^ 1) for i in range(count)]
    across = []
    for sample in range(samples):
        for i in range(1, count - 1, 2):
            across += [(sample * count + i, sample * count + i + 1)]
            across += [(sample * count + i + 1, sample * count + i)]
        partner = sample ^ 1 if samples % 2 == 0 else sample
        for i in (0, count - 1):
            across.append((sample * count + i, partner * count + i))
    return inside, across


def sum_over_gz(part):
    count = lax.axis_size("gz")
    pair = part + lax.ppermute(part, "gz", [(i, i ^ 1) for i in range(count)])
    if count > 8:
        return lax.psum(part, "gz")[None]
    parts = [pair]
    for k in range(1, count // 2):
        parts.append(lax.ppermute(pair, "gz", [(i, (i + 2 * k) % count) for i in range(count)]))
    return jnp.stack(parts)


def on_device(
    field_now,
    field_before,
    lame_lambda,
    shear_modulus,
    density,
    source_field,
    wavelet,
    prior_mean,
    steps_taken,
    grad_change,
):
    depth, rows, cols = shear_modulus.shape
    count = lax.axis_size("gz")
    assert depth == 2 and count % 2 == 0
    inside, across = pairings()
    total = rows // ROWS
    cells = shear_modulus.size
    cuts = [total // 2 + STEPS // 2 - n for n in range(STEPS + 1)]
    wave = jnp.broadcast_to(wavelet[:, None, None], (STEPS, ROWS, LANES))

    def cut_planes(field, tiles):
        cut = tiles * ROWS
        shapes = [(3, cut, cols), (3, rows - cut, cols), (3, rows, cols)]
        low, high, far = call(functools.partial(split_kernel, cut), shapes, [field], cells)
        return [(0, low), (tiles, high)], [(0, far)]

    def across_chips(x):
        return lax.ppermute(x, AXES, across)

    def across_cores(x):
        return lax.ppermute(x, "gz", inside)

    near_now, far_now = cut_planes(field_now, cuts[0])
    ghosts = [(first, across_chips(x)) for first, x in near_now]
    partner = [(0, across_cores(far_now[0][1]))]
    near_old, far_old = cut_planes(field_before, cuts[0] + 1)
    fixed = call(
        coeff_kernel, [shear_modulus.shape] * 3, [lame_lambda, shear_modulus, density], cells * 10
    )
    fixed = list(fixed) + [source_field]
    (static,) = call(dots_kernel, [(DOT_ROWS, LANES)], [steps_taken, grad_change], cells * 40)
    near_sum = far_sum = None
    for n in range(STEPS):
        last = n == STEPS - 1
        middle = cuts[n + 1]
        held = {"f": far_now, "p": near_now, "q": partner, "fb": far_old}
        held |= {} if n == 0 else {"cf": far_sum}
        new_far, sum_far, token = step_call(n, True, 0, total, total, held, wave, fixed, [])
        if not last:
            partner = [(0, across_cores(new_far))]
        held = {"p": near_now[:1], "h": ghosts[:1], "f": far_now, "pb": near_old[:1]}
        held |= {} if n == 0 else {"cp": near_sum[:1]}
        new_low, sum_low, token = step_call(n, False, 0, middle, total, held, wave, fixed, [token])
        if not last:
            low_ghost = across_chips(new_low)
        held = {"p": near_now, "h": ghosts, "f": far_now, "pb": near_old}
        held |= {} if n == 0 else {"cp": near_sum}
        new_high, sum_high, _ = step_call(
            n, False, middle, total, total, held, wave, fixed, [token]
        )
        if not last:
            ghosts = [(0, low_ghost), (middle, across_chips(new_high))]
        near_old, far_old = near_now, far_now
        near_now, far_now = [(0, new_low), (middle, new_high)], [(0, new_far)]
        near_sum, far_sum = [(0, sum_low), (middle, sum_high)], [(0, sum_far)]

    def gradient_dots(so_far, parts):
        operands = [shear_modulus, prior_mean, steps_taken, grad_change, so_far]
        where = [(far, first) for far, first, _ in parts]
        (out,) = call(
            functools.partial(gradient_dots_kernel, where),
            [(DOT_ROWS, LANES)],
            operands + [x for *_, x in parts],
            cells * 20,
        )
        return out

    early = gradient_dots(static, [(True, 0, sum_far), (False, 0, sum_low)])
    mine = gradient_dots(early, [(False, middle, sum_high)])
    final, gradient = call(
        join_kernel,
        [field_now.shape, shear_modulus.shape],
        [new_low, new_high, new_far, sum_low, sum_high, sum_far, shear_modulus, prior_mean],
        cells,
    )
    parts = sum_over_gz(mine)
    (direction,) = call(
        direction_kernel,
        [shear_modulus.shape],
        [parts, gradient, steps_taken, grad_change],
        cells * 20,
    )
    return (final, gradient, direction)


def solution(mesh):
    placed = (
        P("sample", "gz", None, None),
        P("sample", "gz", None, None),
        P("gz", "sample", None),
        P("gz", "sample", None),
        P("gz", "sample", None),
        P("sample", "gz", None, None),
        P("sample"),
        P("gz", "sample", None),
        P("sample", "gz", None, None),
        P("sample", "gz", None, None),
    )
    return jax.shard_map(
        on_device,
        mesh=mesh,
        in_specs=placed,
        out_specs=(P("sample", "gz", None, None), P("gz", "sample", None), P("gz", "sample", None)),
        check_vma=False,
    )
```
